128 devices in a mesh: rep: 8 (over z, y_lo), fsdp: 16 (over y_hi, x, core).
Axes of the slice: x: 4, y: 4 (y_hi: 2, y_lo: 2; y = y_hi * 2 + y_lo), z: 4, core: 2. Of those that a mesh axis runs over, the one named last changes fastest.
Arguments:
- tokens: bfloat16 [65536, 2048], P(('rep', 'fsdp')), may hold values from -6 to 6
- norm_gain: float32 [2048], replicated, may hold values from 0.5 to 1.5
- outer_params: float32 [2, 2048, 4096], P(None, 'fsdp'), may hold values from -6 to 6
- momentum: float32 [2, 2048, 4096], P(None, 'fsdp'), may hold values from -6 to 6
- deltas: bfloat16 [8, 2, 2048, 4096], P('rep', None, 'fsdp'), may hold values from -6 to 6
Outputs:
- new_params: float32 [2, 2048, 4096], P(None, 'fsdp')
- new_momentum: float32 [2, 2048, 4096], P(None, 'fsdp')
- hidden: bfloat16 [65536, 4096], P(('rep', 'fsdp'))
The draws below stay inside these ranges and needn't reach their ends.
All inputs are finite; a program needn't handle non-finite values.
Results may differ from the reference program's by a relative error of at most 0.01.
Values may be sent and summed in bfloat16 or wider, within the bound.
No kernel may reach another device: no remote copies, remote signals or barrier semaphores. Data moves between devices by JAX's collectives and lax.ppermute only.
A program may use at most 192 MiB of HBM per device.

```python
import math
import jax
import jax.numpy as jnp
from jax import lax

D = 2048
FF = 4096
TOKENS = 65536
N_REP = 8


def block_levels(stream_key, shape, split, least, largest):
    def one(position, blocks):
        heights = jax.random.uniform(jax.random.fold_in(jax.random.fold_in(stream_key, 6), position), (blocks,), jnp.float32, least / len(split), largest / len(split))
        return jnp.repeat(jnp.exp(heights), shape[position] // blocks).reshape((-1,) + (1,) * (len(shape) - position - 1))

    loudness = one(*split[0])
    for cut in split[1:]:
        loudness = loudness * one(*cut)
    return loudness


def normal_values(stream_key, dims, deviation, most, pieces=(), held_as=jnp.bfloat16):
    values = jax.random.normal(stream_key, dims, jnp.float32) * deviation
    if len(pieces) > 0:
        values = block_levels(stream_key, dims, pieces, -0.22, 0.18) * values
    return jnp.clip(values, min=-most, max=most).astype(held_as)


def setup_inputs(seed: int = 0) -> dict:
    key_list = jax.random.split(jax.random.key(seed), 6)
    return {
        "tokens": normal_values(key_list[0], (TOKENS, D), 1.0, 6.0, ((0, 128),)),
        "norm_gain": jnp.clip(1.0 + 0.1 * jax.random.normal(key_list[1], (D,), jnp.float32), 0.5, 1.5),
        "outer_params": normal_values(key_list[2], (2, D, FF), 1.0, 6.0, ((1, 16),), jnp.float32),
        "momentum": normal_values(key_list[3], (2, D, FF), 0.5, 6.0, ((1, 16),), jnp.float32),
        "deltas": normal_values(key_list[4], (N_REP, 2, D, FF), 0.5, 6.0, ((0, 8), (2, 16))),
    }


EPS = 1e-05
MU = 0.9
RATE = 0.7

def reference(tokens, norm_gain, outer_params, momentum, deltas):
    total = jnp.zeros(outer_params.shape, jnp.float32)
    for group in range(N_REP):
        total = total + deltas[group].astype(jnp.float32)
    outer_grad = total / N_REP
    new_momentum = MU * momentum + outer_grad
    new_params = outer_params - RATE * (outer_grad + MU * new_momentum)
    weights = new_params.astype(jnp.bfloat16)
    values = tokens.astype(jnp.float32)
    scale_rows = lax.rsqrt(lax.optimization_barrier(jnp.mean(values * values, axis=-1, keepdims=True)) + EPS)
    normed = (values * scale_rows * norm_gain).astype(jnp.bfloat16)
    factor = 1.0 / math.sqrt(D)
    gate = jnp.dot(normed, weights[0], preferred_element_type=jnp.float32) * factor
    up = jnp.dot(normed, weights[1], preferred_element_type=jnp.float32) * factor
    hidden = (jax.nn.silu(gate) * up).astype(jnp.bfloat16)
    return (new_params, new_momentum, hidden)
```

```python
import math

import jax
import jax.numpy as jnp
from jax import lax
from jax.experimental import pallas as pl
from jax.experimental.pallas import tpu as pltpu
from jax.sharding import PartitionSpec as P


EPS = 1e-05
MU = 0.9
RATE = 0.7

AXES = ("rep", "fsdp")
BLK = 256


def permute(value, target):
    pairs = []
    for z in range(4):
        for yl in range(2):
            for yh in range(2):
                for x in range(4):
                    for c in range(2):
                        z2, y2, x2, c2 = target(z, 2 * yh + yl, x, c)
                        z2, y2, x2 = z2 % 4, y2 % 4, x2 % 4
                        here = (((z * 2 + yl) * 2 + yh) * 4 + x) * 2 + c
                        there = (((z2 * 2 + y2 % 2) * 2 + y2 // 2) * 4 + x2) * 2 + c2
                        pairs.append((here, there))
    return lax.ppermute(value, AXES, pairs)


def decode(place):
    code = place[0]
    c = code % 2
    x = (code // 2) % 4
    yh = (code // 8) % 2
    yl = (code // 16) % 2
    z = code // 32
    return z, yl, yh, x, c


def column_block(z, yl, c):
    return (((z % 2) * 2 + c) * 2 + z // 2) * 2 + yl


ANY = pl.BlockSpec(memory_space=pl.ANY)
SMEM = pl.BlockSpec(memory_space=pltpu.SMEM)
SHIFTS = [(dz, dy) for dz in range(4) for dy in range(2)]


def pack_kernel(place, deltas, *refs):
    outs, held, sems = refs[:8], refs[8], refs[9]
    z, yl, _, _, _ = decode(place)
    loads, stores = [], []
    for k, (dz, dy) in enumerate(SHIFTS):
        for c in range(2):
            block = column_block((z + dz) % 4, (yl + dy) % 2, c)
            columns = pl.ds(pl.multiple_of(block * BLK, BLK), BLK)
            loads.append(pltpu.make_async_copy(deltas.at[:, :, columns], held.at[k, c], sems.at[2 * k + c]))
        stores.append(pltpu.make_async_copy(held.at[k], outs[k], sems.at[16 + k]))
    order = list(range(1, 8)) + [0]
    for k in order:
        loads[2 * k].start()
        loads[2 * k + 1].start()
    for k in order:
        loads[2 * k].wait()
        loads[2 * k + 1].wait()
        stores[k].start()
    for store in stores:
        store.wait()


def pack(place, deltas):
    rows = deltas.shape[1]
    return pl.pallas_call(
        pack_kernel,
        in_specs=[SMEM, ANY],
        out_specs=[ANY] * 8,
        out_shape=[jax.ShapeDtypeStruct((2, 2, rows, BLK), deltas.dtype)] * 8,
        scratch_shapes=[pltpu.VMEM((8, 2, 2, rows, BLK), deltas.dtype), pltpu.SemaphoreType.DMA((24,))],
        name="pack",
    )(place, deltas)


def advance(params, moment, outer_grad):
    moment_next = MU * moment + outer_grad
    return params - RATE * (outer_grad + MU * moment_next), moment_next


def reduce_kernel(place, *refs):
    parts, outer, moment, sums, keep, give = refs[:8], refs[8], refs[9], refs[10], refs[11], refs[12]
    total = parts[0][0].astype(jnp.float32)
    for part in parts[1:]:
        total = total + part[0].astype(jnp.float32)
    rounded = total.astype(jnp.bfloat16)
    sums[0] = rounded
    params, _ = advance(outer[...], moment[...], rounded.astype(jnp.float32) * 0.125)
    weights = params.astype(jnp.bfloat16)

    @pl.when(pl.program_id(0) == 0)
    def _():
        give[:, :BLK] = weights[0]
        give[:, BLK:] = weights[1]

    @pl.when(pl.program_id(0) == 1)
    def _():
        keep[:, :BLK] = weights[0]
        keep[:, BLK:] = weights[1]


def reduce_update(place, parts, outer, moment):
    rows = outer.shape[1]

    def core(j, place):
        return 1 - (place[0] + j) % 2

    def columns(j, place):
        z, yl, _, _, _ = decode(place)
        return (0, 0, column_block(z, yl, core(j, place)))

    piece = pl.BlockSpec((1, 2, rows, BLK), lambda j, place: (core(j, place), 0, 0, 0))
    state = pl.BlockSpec((2, rows, BLK), columns)
    whole = pl.BlockSpec((rows, 2 * BLK), lambda j, place: (0, 0))
    shape = jax.ShapeDtypeStruct((rows, 2 * BLK), jnp.bfloat16)
    return pl.pallas_call(
        reduce_kernel,
        grid_spec=pltpu.PrefetchScalarGridSpec(
            num_scalar_prefetch=1,
            grid=(2,),
            in_specs=[piece] * 8 + [state, state],
            out_specs=[piece, whole, whole],
        ),
        out_shape=[jax.ShapeDtypeStruct((2, 2, rows, BLK), jnp.bfloat16), shape, shape],
        name="reduce_update",
    )(place, *parts, outer, moment)


def finish_kernel(place, sums, outer, moment, params_out, moment_out):
    _, yl, _, _, _ = decode(place)
    low = jnp.where(yl == 0, sums[0, 0, 0], sums[0, 1, 0]).astype(jnp.float32)
    high = jnp.where(yl == 0, sums[0, 1, 0], sums[0, 0, 0]).astype(jnp.float32)
    for half, total in enumerate((low, high)):
        at = (slice(None), slice(None), slice(half * BLK, (half + 1) * BLK))
        params_out[at], moment_out[at] = advance(outer[at], moment[at], total * 0.125)


def finish(place, sums, outer, moment):
    rows = outer.shape[1]

    def columns(i, c, place):
        z = (decode(place)[0] + i) % 4
        return (0, 0, ((z % 2) * 2 + c) * 2 + z // 2)

    state = pl.BlockSpec((2, rows, 2 * BLK), columns)
    return pl.pallas_call(
        finish_kernel,
        grid_spec=pltpu.PrefetchScalarGridSpec(
            num_scalar_prefetch=1,
            grid=(4, 2),
            in_specs=[pl.BlockSpec((1, 2, 1, 2, rows, BLK), lambda i, c, place: (i, 0, c, 0, 0, 0)), state, state],
            out_specs=[state, state],
        ),
        out_shape=[jax.ShapeDtypeStruct(outer.shape, jnp.float32)] * 2,
        name="finish",
    )(place, sums, outer, moment)


def project_kernel(factor, count, place, *refs):
    tokens, first, second = refs[:count], refs[count : count + 4], refs[count + 4 : count + 8]
    outs, weights, sems = refs[count + 8 : 2 * count + 8], refs[-2], refs[-1]
    z, yl, yh, x, c = decode(place)
    y = 2 * yh + yl
    copies = [[], [], [], []]
    for i in range(4):
        for j in range(4):
            for k in range(2):
                core = (c + k) % 2
                for group in range(2):
                    dx, dy = (i, j) if group == 0 else (j, i)
                    row = (((y + dy) % 4) // 2) * 8 + ((x + dx) % 4) * 2 + core
                    block = 2 * group + dy % 2
                    source = (first, second)[group][i].at[j, k]
                    target = weights.at[block, pl.ds(pl.multiple_of(row * 128, 128), 128), :]
                    copies[block].append(pltpu.make_async_copy(source, target, sems.at[block, len(copies[block])]))
    for group in copies:
        for copy in group:
            copy.start()
    for block in range(4):
        for copy in copies[block]:
            copy.wait()
        zh = (z // 2 + block // 2) % 2
        at = zh * 2 + (yl + block) % 2
        for t in range(count):
            both = jnp.dot(tokens[t][...], weights[block], preferred_element_type=jnp.float32) * factor
            gate, up = both[:, :BLK], both[:, BLK:]
            hidden = (gate / (1.0 + jnp.exp(-gate)) * up).astype(jnp.bfloat16)
            outs[t][:, pl.ds(pl.multiple_of(at * BLK, BLK), BLK)] = hidden


def project(place, tokens, first, second):
    count, width = tokens[0].shape
    vmem = pl.BlockSpec(memory_space=pltpu.VMEM)
    return pl.pallas_call(
        lambda *refs: project_kernel(1.0 / math.sqrt(width), len(tokens), *refs),
        in_specs=[SMEM] + [vmem] * len(tokens) + [ANY] * 8,
        out_specs=[vmem] * len(tokens),
        out_shape=[jax.ShapeDtypeStruct((count, 4 * BLK), jnp.bfloat16)] * len(tokens),
        scratch_shapes=[pltpu.VMEM((4, width, 2 * BLK), jnp.bfloat16), pltpu.SemaphoreType.DMA((4, 16))],
        name="project",
    )(place, *tokens, *first, *second)


def fill_kernel(kinds, place, *refs):
    count = len(kinds)
    pieces, out, held, sems = refs[:count], refs[-3], refs[-2], refs[-1]
    z, _, _, _, c = decode(place)
    p = z % 2
    loads, stores = [], []
    for k, (same_p, same_c) in enumerate(kinds):
        block = 2 * (p if same_p else 1 - p) + (c if same_c else 1 - c)
        columns = pl.ds(pl.multiple_of(block * 4 * BLK, 4 * BLK), 4 * BLK)
        loads.append(pltpu.make_async_copy(pieces[k], held.at[k], sems.at[0, k]))
        stores.append(pltpu.make_async_copy(held.at[k], out.at[:, columns], sems.at[1, k]))
    for load in loads:
        load.start()
    for load, store in zip(loads, stores):
        load.wait()
        store.start()
    for store in stores:
        store.wait()


def fill(place, pieces, kinds, whole=None):
    count, width = pieces[0].shape
    given = [] if whole is None else [whole]
    return pl.pallas_call(
        lambda *refs: fill_kernel(kinds, *refs),
        in_specs=[SMEM] + [ANY] * (len(pieces) + len(given)),
        out_specs=ANY,
        out_shape=jax.ShapeDtypeStruct((count, 4 * width), pieces[0].dtype),
        input_output_aliases={1 + len(pieces): 0} if given else {},
        scratch_shapes=[
            pltpu.VMEM((len(pieces), count, width), pieces[0].dtype),
            pltpu.SemaphoreType.DMA((2, len(pieces))),
        ],
        name="fill",
    )(place, *pieces, *given)


def along_x(value):
    return [value] + [permute(value, lambda z, y, x, c, d=d: (z, y, x - d, c)) for d in (1, 2, 3)]


def along_y(value):
    return [value] + [permute(value, lambda z, y, x, c, d=d: (z, y - d, x, c)) for d in (1, 2, 3)]


def along_z(value):
    return [value] + [permute(value, lambda z, y, x, c, d=d: (z - d, y, x, c)) for d in (1, 2, 3)]


def other_core(value):
    return permute(value, lambda z, y, x, c: (z, y, x, 1 - c))


def after(value, *others):
    return lax.optimization_barrier((value,) + others)[0]


def step(tokens, norm_gain, outer_params, momentum, deltas):
    place = lax.axis_index(AXES).astype(jnp.int32).reshape(1)
    packed = pack(place, deltas[0])
    parts = [
        permute(piece, lambda z, y, x, c, dz=dz, dy=dy: (z + dz, y ^ dy, x, c))
        for piece, (dz, dy) in zip(packed[1:], SHIFTS[1:])
    ]

    values = tokens.astype(jnp.float32)
    scale_rows = lax.rsqrt(jnp.mean(values * values, axis=-1, keepdims=True) + EPS)
    normed = (values * scale_rows * norm_gain).astype(jnp.bfloat16)
    partner = other_core(after(normed, packed[0]))

    own_part = after(packed[0], normed)
    sums, keep, give = reduce_update(place, [own_part] + parts, outer_params, momentum)
    share = jnp.stack([keep, other_core(give)])

    far = permute(share, lambda z, y, x, c: (z + 2, y, x, c))
    first_own = jnp.stack(along_y(share))
    second_own = jnp.stack(along_x(far))
    first = along_x(first_own)
    second = along_y(second_own)

    pair = jnp.stack([sums, permute(after(sums, share), lambda z, y, x, c: (z, y ^ 1, x, c))])
    pair = after(pair, second_own)
    all_sums = jnp.stack(along_z(pair))
    new_params, new_momentum = finish(place, all_sums, outer_params, momentum)

    straight = permute(after(normed, second_own), lambda z, y, x, c: (z - 1 + 2 * c, y, x, c))
    crossed = other_core(after(straight, new_params))

    (straight,) = project(place, [straight], first, second)
    (crossed,) = project(place, [after(crossed, straight)], first, second)
    partner, own = project(place, [after(partner, crossed), normed], first, second)
    straight = permute(straight, lambda z, y, x, c: (z + 1 - 2 * c, y, x, c))
    crossed = permute(crossed, lambda z, y, x, c: (z - 1 + 2 * c, y, x, 1 - c))
    partner = other_core(partner)
    hidden = fill(place, [own, partner], [(True, True), (True, False)])
    hidden = fill(place, [straight], [(False, True)], hidden)
    hidden = fill(place, [crossed], [(False, False)], hidden)
    return (new_params, new_momentum, hidden)


def solution(mesh):
    in_specs = (
        P(("rep", "fsdp"), None),
        P(),
        P(None, "fsdp", None),
        P(None, "fsdp", None),
        P("rep", None, "fsdp", None),
    )
    out_specs = (P(None, "fsdp", None), P(None, "fsdp", None), P(("rep", "fsdp"), None))
    return jax.shard_map(step, mesh=mesh, in_specs=in_specs, out_specs=out_specs, check_vma=False)
```
